32 devices in a mesh: group: 2 (over x), tile: 16 (over z, y, core).
Axes of the slice: x: 2, y: 2, z: 4, core: 2. Of those that a mesh axis runs over, the one named last changes fastest.
Arguments:
- latents: bfloat16 [384, 16, 128], P(('group', 'tile')), parts along dimension 0, may hold values from -6 to 6
- clip_index: int32 [8], P('group'), parts along dimension 0, may hold values from 0 to 1, never falling along the last dimension, each value on 1 to 3 neighbouring positions
- first_conv: bfloat16 [3, 3, 3, 16, 384], replicated, may hold values from -0.3125 to 0.3125
- first_gain: float32 [384], replicated, may hold values from 0.4 to 1.6
- middle_conv: bfloat16 [3, 3, 3, 384, 384], replicated, may hold values from -0.0625 to 0.0625
- head_gain: float32 [384], replicated, may hold values from 0.4 to 1.6
- head_weight: bfloat16 [384, 48], replicated, may hold values from -0.3125 to 0.3125
Outputs:
- pixels: float32 [32, 2, 3, 48, 128], P(('group', 'tile')), parts along dimension 0
The draws below stay inside these ranges and needn't reach their ends.
There are 2 independent parts, one for each index of `group`. The reference program is written for one: setup_inputs(seed, part) draws one part's arguments, and reference() takes and returns one part's arrays. A program takes and returns all parts, laid end to end along the dimension named above; an argument that names none is the same for every part. Nothing has to cross between parts.
Inputs may be any that keep to these rules, and one draw needn't show every extreme that they name: `clip_index`: clip numbers never fall along the frames; each clip holds 1 to 3 consecutive frames.
All inputs are finite; a program needn't handle non-finite values.
Results may differ from the reference program's by a relative error of at most 0.01.
Values may be sent and summed in bfloat16 or wider, within the bound.
No kernel may reach another device: no remote copies, remote signals or barrier semaphores. Data moves between devices by JAX's collectives and lax.ppermute only.
A program may use at most 128 MiB of HBM per device.

```python
import math
import jax
import jax.numpy as jnp
import numpy as np
from jax import lax

CLAT = 16
CH = 384
PATCH = 16
STRIPS = 8
TF = 2
WS = 16
HL = 48
BLOCKS = 2
TILES = 16
FRAMES = 4
WL = 128
CLIPS = 2
CLIP_MOST = 3


def block_levels(rng, extent, pieces, smallest, top_value):
    def one(axis_at, shards_of):
        draws = jax.random.uniform(jax.random.fold_in(jax.random.fold_in(rng, 6), axis_at), (shards_of,), jnp.float32, smallest / len(pieces), top_value / len(pieces))
        return jnp.repeat(jnp.exp(draws), extent[axis_at] // shards_of).reshape((-1,) + (1,) * (len(extent) - axis_at - 1))

    loudness = one(*pieces[0])
    for cut in pieces[1:]:
        loudness = loudness * one(*cut)
    return loudness


def profile(count, total, most, slope):
    portions = [(1 << 20) // math.isqrt(standing ** slope) + 1 for standing in range(2, count + 1)]
    spare, counts = total - most - (count - 1), [1] * (count - 1)
    while spare > 0:
        candidates = [i for i in range(count - 1) if counts[i] < most]
        pool, left = sum([portions[i] for i in candidates]), spare
        for i in candidates:
            more = min(most - counts[i], max(1, left * portions[i] // pool), spare)
            counts[i] = counts[i] + more
            spare = spare - more
    return np.array([most] + counts)


def uneven_parts(own_key, count, total, most, skew):
    if count == 2:
        one = jax.random.randint(own_key, (), max(1, total - most), min(most, total - 1) + 1)
        return jnp.stack([one, total - one])
    tallies = jnp.asarray(profile(count, total, most, skew), jnp.int32)
    pairs = (count - 1) // 2
    giver, taker = tallies[1:1 + 2 * pairs:2], tallies[2:2 + 2 * pairs:2]
    room = jnp.minimum(giver - 1, most - taker)
    moved = jax.random.randint(jax.random.fold_in(own_key, 1), (pairs,), 0, 1 << 20) % (room + 1)
    tallies = tallies.at[1:1 + 2 * pairs:2].set(giver - moved).at[2:2 + 2 * pairs:2].set(taker + moved)
    return tallies[jax.random.permutation(jax.random.fold_in(own_key, 2), count)]


def bell_draw(own_key, shape, scale, limit, cuts=(), kind=jnp.bfloat16):
    drawn = scale * jax.random.normal(own_key, shape, jnp.float32)
    if cuts:
        drawn = drawn * block_levels(own_key, shape, cuts, -0.22, 0.18)
    return jnp.clip(drawn, -limit, limit).astype(kind)


def setup_inputs(seed: int = 0, part: int = 0) -> dict:
    key_of = jax.random.split(jax.random.key(seed), 8)
    part_splits = jax.random.split(jax.random.fold_in(key_of[7], part), 8)
    return {
        "latents": bell_draw(part_splits[0], (FRAMES * HL, CLAT, WL), 1.0, 6.0, ((0, 16),)),
        "clip_index": jnp.searchsorted(jnp.cumsum(uneven_parts(part_splits[1], CLIPS, FRAMES, CLIP_MOST, 1)), jnp.arange(FRAMES), side="right").astype(jnp.int32),
        "first_conv": bell_draw(key_of[2], (3, 3, 3, CLAT, CH), (27 * CLAT) ** -0.5, 0.3125),
        "first_gain": jnp.clip(1.0 + 0.12 * jax.random.normal(key_of[3], (CH,), jnp.float32), 0.4, 1.6),
        "middle_conv": bell_draw(key_of[4], (3, 3, 3, CH, CH), (27 * CH) ** -0.5, 0.0625),
        "head_gain": jnp.clip(1.0 + 0.12 * jax.random.normal(key_of[5], (CH,), jnp.float32), 0.4, 1.6),
        "head_weight": bell_draw(key_of[6], (CH, 3 * PATCH), CH ** -0.5, 0.3125),
    }


def causal_conv(field, clip_index, weight):
    frames, height, width, channels = field.shape
    outs = weight.shape[-1]
    ids = jnp.concatenate([jnp.full((2,), -1, jnp.int32), clip_index.astype(jnp.int32)])
    padded = jnp.pad(field, ((2, 0), (1, 1), (1, 1), (0, 0)))
    total = jnp.zeros((frames * height * width, outs), jnp.float32)
    for step_t in range(3):
        keep = (ids[step_t:step_t + frames] == ids[2:]).astype(field.dtype)
        slab = padded[step_t:step_t + frames] * keep[:, None, None, None]
        for step_r in range(3):
            rows = slab[:, step_r:step_r + height]
            stacked = jnp.concatenate([rows[:, :, step_c:step_c + width] for step_c in range(3)], axis=-1)
            stacked = stacked.reshape(-1, 3 * channels)
            total = total + jnp.dot(stacked, weight[step_t, step_r].reshape(3 * channels, outs), preferred_element_type=jnp.float32)
    return total.reshape(frames, height, width, outs)

def norm_act(values, gain):
    scale = lax.rsqrt(lax.optimization_barrier(jnp.mean(values * values, axis=-1, keepdims=True)) + 1e-06)
    return jax.nn.silu(values * scale * gain.astype(jnp.float32))

def reference(latents, clip_index, first_conv, first_gain, middle_conv, head_gain, head_weight):
    video = latents.reshape(FRAMES, HL, CLAT, WL).transpose(0, 1, 3, 2)
    first = causal_conv(video, clip_index, first_conv).astype(jnp.bfloat16)
    active = norm_act(first.astype(jnp.float32), first_gain).astype(jnp.bfloat16)
    summed = first.astype(jnp.float32) + causal_conv(active, clip_index, middle_conv)
    outward = norm_act(summed, head_gain).astype(jnp.bfloat16)
    patch = jnp.dot(outward.reshape(-1, CH), head_weight, preferred_element_type=jnp.float32)
    patch = patch.reshape(FRAMES, HL, WL, 3, PATCH)
    half = PATCH // 2
    front = patch[..., :half]
    back = patch[..., half:]
    moved = jnp.concatenate([jnp.zeros_like(back[:, :, :1]), back[:, :, :-1]], axis=2)
    picture = front + moved
    tiles = picture.reshape(BLOCKS, TF, HL, STRIPS, WS, 3, half)
    tiles = tiles.transpose(0, 3, 1, 5, 2, 4, 6)
    tiles = tiles.reshape(TILES, TF, 3, HL, WS * half)
    return jnp.roll(tiles, STRIPS // 2 - 1, axis=0)
```

```python
import functools

import jax
import jax.numpy as jnp
from jax import lax
from jax.experimental import pallas as pl
from jax.experimental.pallas import tpu as pltpu
from jax.sharding import PartitionSpec as P

CLAT = 16
CH = 384
PATCH = 16
STRIPS = 8
TF = 2
WS = 16
HL = 48
LANE = 128
PER_TILE = LANE // CLAT
TILES_WIN = 4
PAIRS = 10
COLS = 2 * PAIRS
OUT_COLS = WS + 1
CELLS = PAIRS * HL
OUT_CELLS = OUT_COLS * HL
PAD = 8
LT = CH // LANE


def silu(v):
    half = 0.5 * v
    return half + half * jnp.tanh(half)


def inv_rms(x):
    return lax.rsqrt(jnp.mean(x * x, axis=-1, keepdims=True) + 1e-06)


def decode_kernel(
    slots,
    place_ref,
    clip_ref,
    recv_ref,
    fc_ref,
    fg_ref,
    mc_ref,
    hg_ref,
    hw_ref,
    out_ref,
    wbuf,
    b1,
    vf,
    x1,
    act,
    first,
    xw,
    ysum,
    wsem,
):
    f32, bf16 = jnp.float32, jnp.bfloat16
    copies = []
    for dt, dest in ((0, 0), (1, 1), (2, 3)):
        for dr in range(3):
            for dc in range(3):
                copy = pltpu.make_async_copy(
                    mc_ref.at[dt, dr, dc],
                    wbuf.at[dest, pl.ds((dc * 3 + dr) * CH, CH)],
                    wsem.at[dt * 9 + dr * 3 + dc],
                )
                copy.start()
                copies.append(copy)

    place = place_ref[0]
    tiles = recv_ref.shape[0]
    rotated = lax.rem(place - (STRIPS // 2 - 1) + tiles, tiles)
    column = lax.rem(rotated, STRIPS)
    block = lax.div(rotated, STRIPS)
    ids = []
    for slot in range(6):
        frame = block * TF - 4 + slot
        known = clip_ref[jnp.maximum(frame, 0)]
        ids.append(jnp.where(frame >= 0, known, -1))
    inner_left = jnp.where(column > 0, 1.0, 0.0).astype(f32)
    inner_right = jnp.where(column < STRIPS - 1, 1.0, 0.0).astype(f32)

    b1[...] = jnp.zeros_like(b1)
    for dt in range(3):
        for dr in range(3):
            taps = fc_ref[dt * 3 + dr]
            b1[dt, dr * 64 : dr * 64 + 48, :CH] = taps
            b1[dt, dr * 64 + 16 : dr * 64 + 64, CH:] = taps

    vf[...] = jnp.zeros_like(vf)
    for slot in range(6 - slots, 6):
        base = jnp.maximum(block * TF - 4 + slot, 0) * 4
        for quarter in range(4):
            for tile in range(TILES_WIN):
                vf[PAD + 12 * quarter : PAD + 12 * quarter + 12, tile * LANE : (tile + 1) * LANE] = (
                    recv_ref[base + quarter, tile].astype(f32)
                )
        rows = [vf[PAD - 1 + dr : PAD - 1 + dr + HL, :] for dr in range(3)]
        for pair in range(PAIRS):
            at = 32 * pair + 80
            x1[slot - 6 + slots, pair * HL : (pair + 1) * HL, :] = jnp.concatenate(
                [row[:, at : at + 64] for row in rows], axis=-1
            ).astype(bf16)

    act[...] = jnp.zeros_like(act)
    gain = fg_ref[...]
    for t in range(4):
        total = None
        for dt in range(3):
            slot = t + dt
            if slot < 6 - slots:
                continue
            left = x1[slot - 6 + slots]
            if dt < 2:
                left = left * jnp.where(ids[slot] == ids[t + 2], 1.0, 0.0).astype(bf16)
            part = jnp.dot(left, b1[dt], preferred_element_type=f32)
            total = part if total is None else total + part
        for side in range(2):
            rounded = total[:, side * CH : (side + 1) * CH].astype(bf16)
            if t >= 2:
                for pair in range(PAIRS):
                    first[t - 2, (2 * pair + side) * HL : (2 * pair + side + 1) * HL, :] = rounded[
                        pair * HL : (pair + 1) * HL
                    ]
            x = rounded.astype(f32)
            a = silu(x * inv_rms(x) * gain)
            for pair in range(PAIRS):
                piece = a[pair * HL : (pair + 1) * HL]
                if pair == 0:
                    piece = piece * inner_left
                if pair == PAIRS - 1:
                    piece = piece * inner_right
                for lt in range(LT):
                    act[t, 2 * pair + side, lt, PAD : PAD + HL, :] = piece[:, lt * LANE : (lt + 1) * LANE]

    same = jnp.where(ids[4] == ids[5], 1.0, 0.0).astype(f32)
    keep0 = jnp.where(ids[2] == ids[4], 1.0, 0.0).astype(f32)
    keep1 = jnp.where(ids[3] == ids[4], 1.0, 0.0).astype(f32)
    whole = 1.0 - 0.5 * same
    half = 0.5 * same

    def transform(j, carry):
        at = pl.multiple_of(j * HL, HL)
        for dr in range(3):
            for lt in range(LT):
                d = [act[t, j, lt, PAD - 1 + dr : PAD - 1 + dr + HL, :].astype(bf16).astype(f32) for t in range(4)]
                d1 = d[1] * keep1
                mixed = (
                    d[0] * keep0 - same * d[2],
                    whole * d1 + half * d[2],
                    whole * d[2] - half * d1,
                    d[3] - same * d1,
                )
                lanes = slice((dr * LT + lt) * LANE, (dr * LT + lt + 1) * LANE)
                for m in range(4):
                    xw[m, pl.ds(at, HL), lanes] = mixed[m].astype(bf16)
        return carry

    lax.fori_loop(0, COLS, transform, 0)

    for copy in copies:
        copy.wait()

    def weights(i, carry):
        at = pl.multiple_of(i * LANE, LANE)
        g0 = wbuf[0, pl.ds(at, LANE), :].astype(f32)
        g1 = wbuf[1, pl.ds(at, LANE), :].astype(f32)
        g2 = wbuf[3, pl.ds(at, LANE), :].astype(f32)
        wbuf[1, pl.ds(at, LANE), :] = (g1 + same * (g0 + g2)).astype(bf16)
        wbuf[2, pl.ds(at, LANE), :] = (g2 + same * (g0 - g1)).astype(bf16)
        return carry

    lax.fori_loop(0, 9 * CH // LANE, weights, 0)

    ysum[...] = jnp.zeros_like(ysum)

    def products(m, carry):
        left = jnp.concatenate(
            [xw[m, (1 + dc - 1) * HL : (1 + dc - 1) * HL + OUT_CELLS, :] for dc in range(3)], axis=-1
        )
        part = jnp.dot(left, wbuf[m], preferred_element_type=f32)
        scale0 = jnp.where(m < 3, 1.0, 0.0).astype(f32)
        sign = jnp.where(m == 1, same, jnp.where(m == 2, -same, 0.0))
        scale1 = jnp.where(m == 3, 1.0, sign).astype(f32)
        ysum[0] += part * scale0
        ysum[1] += part * scale1
        return carry

    lax.fori_loop(0, 4, products, 0)

    hgain = hg_ref[...]
    lane = lax.broadcasted_iota(jnp.int32, (HL, LANE), 1)
    for t in range(2):
        x = ysum[t] + first[t, HL : HL + OUT_CELLS, :].astype(f32)
        outward = silu(x * inv_rms(x) * hgain).astype(bf16)
        patch = jnp.dot(outward, hw_ref[...], preferred_element_type=f32)
        for colour in range(3):
            sums = [jnp.zeros((HL, LANE), f32), jnp.zeros((HL, LANE), f32)]
            for w in range(-1, WS):
                cell = patch[(w + 1) * HL : (w + 2) * HL]
                if w < 0:
                    cell = cell * inner_left
                turned = pltpu.roll(cell, (8 * w - PATCH * colour) % LANE, 1)
                inside = (lane >= 8 * w) & (lane < 8 * w + PATCH)
                sums[w % 2] = jnp.where(inside, turned, sums[w % 2])
            out_ref[0, t, colour] = sums[0] + sums[1]


def per_device(latents, clip_index, first_conv, first_gain, middle_conv, head_gain, head_weight):
    tiles = lax.axis_size("tile")
    place = lax.axis_index("tile").astype(jnp.int32).reshape(1)
    rows = latents.shape[0]
    width = latents.shape[2]
    blocks = tiles // STRIPS
    slots = min(6, blocks * TF)
    packed = latents.reshape(rows, CLAT, width // PER_TILE, PER_TILE).transpose(2, 0, 3, 1)
    packed = packed.reshape(width // PER_TILE, rows, LANE)
    packed = jnp.pad(packed, ((1, 1), (0, 0), (0, 0)))
    sent = []
    for dest in range(tiles):
        strip = (dest - (STRIPS // 2 - 1)) % tiles % STRIPS
        sent.append(packed[2 * strip : 2 * strip + TILES_WIN])
    sent = jnp.stack(sent)
    came = lax.all_to_all(sent, "tile", 0, 0, tiled=True)

    vmem = pl.BlockSpec(memory_space=pltpu.VMEM)
    smem = pl.BlockSpec(memory_space=pltpu.SMEM)
    call = pl.pallas_call(
        functools.partial(decode_kernel, slots),
        out_shape=jax.ShapeDtypeStruct((1, TF, 3, HL, WS * PATCH // 2), jnp.float32),
        in_specs=[smem, smem, vmem, vmem, vmem, pl.BlockSpec(memory_space=pl.ANY), vmem, vmem],
        out_specs=vmem,
        scratch_shapes=[
            pltpu.VMEM((4, 9 * CH, CH), jnp.bfloat16),
            pltpu.VMEM((3, 192, 2 * CH), jnp.bfloat16),
            pltpu.VMEM((HL + 2 * PAD, TILES_WIN * LANE), jnp.float32),
            pltpu.VMEM((slots, CELLS, 192), jnp.bfloat16),
            pltpu.VMEM((4, COLS, LT, HL + 2 * PAD, LANE), jnp.float32),
            pltpu.VMEM((2, COLS * HL, CH), jnp.bfloat16),
            pltpu.VMEM((4, COLS * HL, 3 * CH), jnp.bfloat16),
            pltpu.VMEM((2, OUT_CELLS, CH), jnp.float32),
            pltpu.SemaphoreType.DMA((27,)),
        ],
        compiler_params=pltpu.CompilerParams(vmem_limit_bytes=60 * 1024 * 1024),
    )
    return call(
        place,
        clip_index,
        came,
        first_conv.reshape(9, 3 * CLAT, CH),
        first_gain.reshape(1, CH),
        middle_conv,
        head_gain.reshape(1, CH),
        jnp.pad(head_weight, ((0, 0), (0, LANE - 3 * PATCH))),
    )


def solution(mesh):
    placed = (P(("group", "tile"), None, None), P("group"), P(), P(), P(), P(), P())
    return jax.shard_map(
        per_device,
        mesh=mesh,
        in_specs=placed,
        out_specs=P(("group", "tile"), None, None, None, None),
        check_vma=False,
    )
```

```python
import functools

import jax
import jax.numpy as jnp
from jax import lax
from jax.experimental import pallas as pl
from jax.experimental.pallas import tpu as pltpu
from jax.sharding import PartitionSpec as P

CLAT = 16
CH = 384
PATCH = 16
STRIPS = 8
TF = 2
WS = 16
HL = 48
LANE = 128
PER_TILE = LANE // CLAT
TILES_WIN = 4
PAIRS = 10
COLS = 2 * PAIRS
OUT_COLS = WS + 1
CELLS = PAIRS * HL
OUT_CELLS = OUT_COLS * HL
PAD = 8
LT = CH // LANE


def silu(v):
    half = 0.5 * v
    return half + half * jnp.tanh(half)


def inv_rms(x):
    return lax.rsqrt(jnp.mean(x * x, axis=-1, keepdims=True) + 1e-06)


def decode_kernel(
    slots,
    place_ref,
    clip_ref,
    recv_ref,
    fc_ref,
    fg_ref,
    mc_ref,
    hg_ref,
    hw_ref,
    out_ref,
    wbuf,
    b1,
    vf,
    x1,
    act,
    first,
    xw,
    ysum,
    wsem,
):
    f32, bf16 = jnp.float32, jnp.bfloat16
    copies = []
    for dt, dest in ((0, 0), (1, 1), (2, 3)):
        for dr in range(3):
            for dc in range(3):
                copy = pltpu.make_async_copy(
                    mc_ref.at[dt, dr, dc],
                    wbuf.at[dest, pl.ds((dc * 3 + dr) * CH, CH)],
                    wsem.at[dt * 9 + dr * 3 + dc],
                )
                copy.start()
                copies.append(copy)

    place = place_ref[0]
    tiles = recv_ref.shape[0]
    rotated = lax.rem(place - (STRIPS // 2 - 1) + tiles, tiles)
    column = lax.rem(rotated, STRIPS)
    block = lax.div(rotated, STRIPS)
    ids = []
    for slot in range(6):
        frame = block * TF - 4 + slot
        known = clip_ref[jnp.maximum(frame, 0)]
        ids.append(jnp.where(frame >= 0, known, -1))
    inner_left = jnp.where(column > 0, 1.0, 0.0).astype(f32)
    inner_right = jnp.where(column < STRIPS - 1, 1.0, 0.0).astype(f32)

    b1[...] = jnp.zeros_like(b1)
    for dt in range(3):
        for dr in range(3):
            taps = fc_ref[dt * 3 + dr]
            b1[dt, dr * 64 : dr * 64 + 48, :CH] = taps
            b1[dt, dr * 64 + 16 : dr * 64 + 64, CH:] = taps

    vf[...] = jnp.zeros_like(vf)
    for slot in range(6 - slots, 6):
        base = jnp.maximum(block * TF - 4 + slot, 0) * 4
        for quarter in range(4):
            for tile in range(TILES_WIN):
                vf[PAD + 12 * quarter : PAD + 12 * quarter + 12, tile * LANE : (tile + 1) * LANE] = (
                    recv_ref[base + quarter, tile].astype(f32)
                )
        rows = [vf[PAD - 1 + dr : PAD - 1 + dr + HL, :] for dr in range(3)]
        for pair in range(PAIRS):
            at = 32 * pair + 80
            x1[slot - 6 + slots, pair * HL : (pair + 1) * HL, :] = jnp.concatenate(
                [row[:, at : at + 64] for row in rows], axis=-1
            ).astype(bf16)

    act[...] = jnp.zeros_like(act)
    gain = fg_ref[...]
    for t in range(4):
        total = None
        for dt in range(3):
            slot = t + dt
            if slot < 6 - slots:
                continue
            left = x1[slot - 6 + slots]
            if dt < 2:
                left = left * jnp.where(ids[slot] == ids[t + 2], 1.0, 0.0).astype(bf16)
            part = jnp.dot(left, b1[dt], preferred_element_type=f32)
            total = part if total is None else total + part
        for side in range(2):
            rounded = total[:, side * CH : (side + 1) * CH].astype(bf16)
            if t >= 2:
                for pair in range(PAIRS):
                    first[t - 2, (2 * pair + side) * HL : (2 * pair + side + 1) * HL, :] = rounded[
                        pair * HL : (pair + 1) * HL
                    ]
            x = rounded.astype(f32)
            a = silu(x * inv_rms(x) * gain)
            for pair in range(PAIRS):
                piece = a[pair * HL : (pair + 1) * HL]
                if pair == 0:
                    piece = piece * inner_left
                if pair == PAIRS - 1:
                    piece = piece * inner_right
                for lt in range(LT):
                    act[t, 2 * pair + side, lt, PAD : PAD + HL, :] = piece[:, lt * LANE : (lt + 1) * LANE]

    same = jnp.where(ids[4] == ids[5], 1.0, 0.0).astype(f32)
    keep0 = jnp.where(ids[2] == ids[4], 1.0, 0.0).astype(f32)
    keep1 = jnp.where(ids[3] == ids[4], 1.0, 0.0).astype(f32)
    whole = 1.0 - 0.5 * same
    half = 0.5 * same

    def transform(j, carry):
        at = pl.multiple_of(j * HL, HL)
        for dr in range(3):
            for lt in range(LT):
                d = [act[t, j, lt, PAD - 1 + dr : PAD - 1 + dr + HL, :].astype(bf16).astype(f32) for t in range(4)]
                d1 = d[1] * keep1
                mixed = (
                    d[0] * keep0 - same * d[2],
                    whole * d1 + half * d[2],
                    whole * d[2] - half * d1,
                    d[3] - same * d1,
                )
                lanes = slice((dr * LT + lt) * LANE, (dr * LT + lt + 1) * LANE)
                for m in range(4):
                    xw[m, pl.ds(at, HL), lanes] = mixed[m].astype(bf16)
        return carry

    lax.fori_loop(0, COLS, transform, 0)

    for copy in copies:
        copy.wait()

    def weights(i, carry):
        at = pl.multiple_of(i * LANE, LANE)
        g0 = wbuf[0, pl.ds(at, LANE), :].astype(f32)
        g1 = wbuf[1, pl.ds(at, LANE), :].astype(f32)
        g2 = wbuf[3, pl.ds(at, LANE), :].astype(f32)
        wbuf[1, pl.ds(at, LANE), :] = (g1 + same * (g0 + g2)).astype(bf16)
        wbuf[2, pl.ds(at, LANE), :] = (g2 + same * (g0 - g1)).astype(bf16)
        return carry

    lax.fori_loop(0, 9 * CH // LANE, weights, 0)

    ysum[...] = jnp.zeros_like(ysum)

    def products(m, carry):
        left = jnp.concatenate(
            [xw[m, (1 + dc - 1) * HL : (1 + dc - 1) * HL + OUT_CELLS, :] for dc in range(3)], axis=-1
        )
        part = jnp.dot(left, wbuf[m], preferred_element_type=f32)
        scale0 = jnp.where(m < 3, 1.0, 0.0).astype(f32)
        sign = jnp.where(m == 1, same, jnp.where(m == 2, -same, 0.0))
        scale1 = jnp.where(m == 3, 1.0, sign).astype(f32)
        ysum[0] += part * scale0
        ysum[1] += part * scale1
        return carry

    lax.fori_loop(0, 4, products, 0)

    hgain = hg_ref[...]
    lane = lax.broadcasted_iota(jnp.int32, (HL, LANE), 1)
    for t in range(2):
        x = ysum[t] + first[t, HL : HL + OUT_CELLS, :].astype(f32)
        outward = silu(x * inv_rms(x) * hgain).astype(bf16)
        patch = jnp.dot(outward, hw_ref[...], preferred_element_type=f32)
        for colour in range(3):
            sums = [jnp.zeros((HL, LANE), f32), jnp.zeros((HL, LANE), f32)]
            for w in range(-1, WS):
                cell = patch[(w + 1) * HL : (w + 2) * HL]
                if w < 0:
                    cell = cell * inner_left
                turned = pltpu.roll(cell, (8 * w - PATCH * colour) % LANE, 1)
                inside = (lane >= 8 * w) & (lane < 8 * w + PATCH)
                sums[w % 2] = jnp.where(inside, turned, sums[w % 2])
            out_ref[0, t, colour] = sums[0] + sums[1]


def window_kernel(tiles, packed_ref, out_ref):
    for dest in range(tiles):
        strip = (dest - (STRIPS // 2 - 1)) % tiles % STRIPS
        out_ref[dest] = packed_ref[2 * strip : 2 * strip + TILES_WIN]


def per_device(latents, clip_index, first_conv, first_gain, middle_conv, head_gain, head_weight):
    tiles = lax.axis_size("tile")
    place = lax.axis_index("tile").astype(jnp.int32).reshape(1)
    rows = latents.shape[0]
    width = latents.shape[2]
    blocks = tiles // STRIPS
    slots = min(6, blocks * TF)
    packed = latents.reshape(rows, CLAT, width // PER_TILE, PER_TILE).transpose(2, 0, 3, 1)
    packed = packed.reshape(width // PER_TILE, rows, LANE)
    packed = jnp.pad(packed, ((1, 1), (0, 0), (0, 0)))
    sent = pl.pallas_call(
        functools.partial(window_kernel, tiles),
        out_shape=jax.ShapeDtypeStruct((tiles, TILES_WIN, rows, LANE), packed.dtype),
        in_specs=[pl.BlockSpec(memory_space=pltpu.VMEM)],
        out_specs=pl.BlockSpec(memory_space=pltpu.VMEM),
        compiler_params=pltpu.CompilerParams(vmem_limit_bytes=8 * 1024 * 1024),
    )(packed)
    came = lax.all_to_all(sent, "tile", 0, 0, tiled=True)

    vmem = pl.BlockSpec(memory_space=pltpu.VMEM)
    smem = pl.BlockSpec(memory_space=pltpu.SMEM)
    call = pl.pallas_call(
        functools.partial(decode_kernel, slots),
        out_shape=jax.ShapeDtypeStruct((1, TF, 3, HL, WS * PATCH // 2), jnp.float32),
        in_specs=[smem, smem, vmem, vmem, vmem, pl.BlockSpec(memory_space=pl.ANY), vmem, vmem],
        out_specs=vmem,
        scratch_shapes=[
            pltpu.VMEM((4, 9 * CH, CH), jnp.bfloat16),
            pltpu.VMEM((3, 192, 2 * CH), jnp.bfloat16),
            pltpu.VMEM((HL + 2 * PAD, TILES_WIN * LANE), jnp.float32),
            pltpu.VMEM((slots, CELLS, 192), jnp.bfloat16),
            pltpu.VMEM((4, COLS, LT, HL + 2 * PAD, LANE), jnp.float32),
            pltpu.VMEM((2, COLS * HL, CH), jnp.bfloat16),
            pltpu.VMEM((4, COLS * HL, 3 * CH), jnp.bfloat16),
            pltpu.VMEM((2, OUT_CELLS, CH), jnp.float32),
            pltpu.SemaphoreType.DMA((27,)),
        ],
        compiler_params=pltpu.CompilerParams(vmem_limit_bytes=60 * 1024 * 1024),
    )
    return call(
        place,
        clip_index,
        came,
        first_conv.reshape(9, 3 * CLAT, CH),
        first_gain.reshape(1, CH),
        middle_conv,
        head_gain.reshape(1, CH),
        jnp.pad(head_weight, ((0, 0), (0, LANE - 3 * PATCH))),
    )


def solution(mesh):
    placed = (P(("group", "tile"), None, None), P("group"), P(), P(), P(), P(), P())
    return jax.shard_map(
        per_device,
        mesh=mesh,
        in_specs=placed,
        out_specs=P(("group", "tile"), None, None, None, None),
        check_vma=False,
    )
```

```python
import functools

import jax
import jax.numpy as jnp
from jax import lax
from jax.experimental import pallas as pl
from jax.experimental.pallas import tpu as pltpu
from jax.sharding import PartitionSpec as P

CLAT = 16
CH = 384
PATCH = 16
STRIPS = 8
TF = 2
WS = 16
HL = 48
LANE = 128
PER_TILE = LANE // CLAT
TILES_WIN = 3
SKIP = (PER_TILE - 3) * CLAT
PAIRS = 10
COLS = 2 * PAIRS
OUT_COLS = WS + 1
CELLS = PAIRS * HL
OUT_HALF = OUT_COLS * HL // 2
PAD = 8
STEP = 64
LT = CH // LANE


def silu_of_twice(half):
    return half + half * jnp.tanh(half)


def inv_rms(x):
    return lax.rsqrt(jnp.mean(x * x, axis=-1, keepdims=True) + 1e-06)


def position(place_ref, tiles):
    rotated = lax.rem(place_ref[0] - (STRIPS // 2 - 1) + tiles, tiles)
    return lax.rem(rotated, STRIPS), lax.div(rotated, STRIPS)


def frame_ids(clip_ref, block):
    ids = []
    for slot in range(6):
        frame = block * TF - 4 + slot
        known = clip_ref[jnp.maximum(frame, 0)]
        ids.append(jnp.where(frame >= 0, known, -1))
    return ids


def flag(condition):
    return jnp.where(condition, 1.0, 0.0).astype(jnp.float32)


def weights_kernel(tiles, place_ref, clip_ref, mc_ref, fc_ref, out_ref, b1_ref, gbuf, mbuf, insem, outsem):
    f32, bf16 = jnp.float32, jnp.bfloat16
    loads = []
    for dr in range(3):
        load = pltpu.make_async_copy(mc_ref.at[:, dr], gbuf.at[:, dr], insem.at[dr])
        load.start()
        loads.append(load)
    _, block = position(place_ref, tiles)
    ids = frame_ids(clip_ref, block)
    same = flag(ids[4] == ids[5])
    scale = 1.0 - 0.5 * same

    b1_ref[...] = jnp.zeros_like(b1_ref)
    for dt in range(3):
        for dr in range(3):
            for dc in range(3):
                at = dr * 64 + dc * CLAT
                taps = fc_ref[dt, dr, dc]
                b1_ref[dt, at : at + CLAT, :CH] = taps
                b1_ref[dt, at + CLAT : at + 2 * CLAT, CH:] = taps

    stores = []
    for dr in range(3):
        loads[dr].wait()
        for dc in range(3):
            tap = dr * 3 + dc

            def rows(i, carry):
                at = pl.multiple_of(i * STEP, STEP)
                g0, g1, g2 = (gbuf[dt, dr, dc, pl.ds(at, STEP), :].astype(f32) for dt in range(3))
                s0 = same * g0
                mbuf[tap, 0, pl.ds(at, STEP), :] = (scale * (g1 + (s0 + same * g2))).astype(bf16)
                mbuf[tap, 1, pl.ds(at, STEP), :] = (scale * (g2 + (s0 - same * g1))).astype(bf16)
                return carry

            lax.fori_loop(0, CH // STEP, rows, 0)
            for m in range(2):
                store = pltpu.make_async_copy(
                    mbuf.at[tap, m], out_ref.at[m, pl.ds(tap * CH, CH)], outsem.at[tap * 2 + m]
                )
                store.start()
                stores.append(store)
    for store in stores:
        store.wait()


def decode_kernel(
    slots,
    place_ref,
    clip_ref,
    recv_ref,
    b1_ref,
    fg_ref,
    wt_ref,
    mc_ref,
    hg_ref,
    hw_ref,
    out_ref,
    wbuf,
    hbuf,
    hwbuf,
    vf,
    x1,
    act,
    first,
    xa,
    ysum,
    wsem,
):
    f32, bf16 = jnp.float32, jnp.bfloat16
    copies = []
    for m in range(4):
        group = []
        for dr in range(3):
            for dc in range(3):
                tap = pl.ds((dr * 3 + dc) * CH, CH)
                source = mc_ref.at[m // 3 * 2, dr, dc] if m in (0, 3) else wt_ref.at[m - 1, tap]
                copy = pltpu.make_async_copy(source, wbuf.at[m, tap], wsem.at[m * 9 + dr * 3 + dc])
                copy.start()
                group.append(copy)
        copies.append(group)

    column, block = position(place_ref, recv_ref.shape[0])
    ids = frame_ids(clip_ref, block)
    inner_left = flag(column > 0)
    inner_right = flag(column < STRIPS - 1)
    hwbuf[...] = jnp.zeros_like(hwbuf)
    hwbuf[: 3 * PATCH] = hw_ref[...]

    vf[...] = jnp.zeros_like(vf)
    for slot in range(6 - slots, 6):
        base = jnp.maximum(block * TF - 4 + slot, 0) * 4
        for quarter in range(4):
            for tile in range(TILES_WIN):
                vf[PAD + 12 * quarter : PAD + 12 * quarter + 12, tile * LANE : (tile + 1) * LANE] = (
                    recv_ref[base + quarter, 12 * tile : 12 * tile + 12].astype(f32)
                )
        rows = [vf[PAD - 1 + dr : PAD - 1 + dr + HL, :] for dr in range(3)]
        for pair in range(PAIRS):
            at = 32 * pair
            x1[slot - 6 + slots, pair * HL : (pair + 1) * HL, :] = jnp.concatenate(
                [row[:, at : at + 64] for row in rows], axis=-1
            ).astype(bf16)

    for t in range(4):
        for col in range(COLS):
            for lt in range(LT):
                act[t, col, lt, 0:PAD, :] = jnp.zeros((PAD, LANE), f32)
                act[t, col, lt, PAD + HL :, :] = jnp.zeros((PAD, LANE), f32)
    gain = 0.5 * fg_ref[...].reshape(1, CH)
    same = flag(ids[4] == ids[5])
    keeps = [flag(ids[2] == ids[4]), flag(ids[3] == ids[4]), None, None]
    for t in range(4):
        total = None
        for dt in range(3):
            slot = t + dt
            if slot < 6 - slots:
                continue
            left = x1[slot - 6 + slots]
            if dt < 2:
                left = left * flag(ids[slot] == ids[t + 2]).astype(bf16)
            part = jnp.dot(left, b1_ref[dt], preferred_element_type=f32)
            total = part if total is None else total + part
        for side in range(2):
            x = total[:, side * CH : (side + 1) * CH]
            a = silu_of_twice(x * inv_rms(x) * gain)
            if keeps[t] is not None:
                a = a * keeps[t]
            for pair in range(PAIRS):
                cut = slice(pair * HL, (pair + 1) * HL)
                piece = a[cut]
                if pair == 0:
                    piece = piece * inner_left
                if pair == PAIRS - 1:
                    piece = piece * inner_right
                for lt in range(LT):
                    lanes = slice(lt * LANE, (lt + 1) * LANE)
                    act[t, 2 * pair + side, lt, PAD : PAD + HL, :] = piece[:, lanes]
                    if t >= 2:
                        first[t - 2, 2 * pair + side, lt] = x[cut, lanes]

    def transform(pair, carry):
        at = pl.multiple_of(pair * HL, HL)
        for lt in range(LT):
            sides = []
            for side in range(2):
                timed = []
                for k in range(4):
                    d = [act[t, 2 * pair + side, lt, pl.ds(PAD - 1 + k, HL // 2, stride=2), :] for t in range(4)]
                    s1, s2 = same * d[1], same * d[2]
                    timed.append((d[0] - s2, d[1] + s2, d[2] - s1, d[3] - s1))
                mixed = []
                for m in range(4):
                    r0, r1, r2, r3 = (timed[k][m] for k in range(4))
                    mixed += [r0 - r2, r1 + r2, r2 - r1, r1 - r3]
                sides.append(mixed)
            for k in range(16):
                both = jnp.concatenate([sides[0][k], sides[1][k]], axis=0).astype(bf16)
                xa[k, pl.ds(at, HL), lt * LANE : (lt + 1) * LANE] = both
        return carry

    lax.fori_loop(0, PAIRS, transform, 0, unroll=2)

    deep = 3 * CH
    for m in range(4):
        for copy in copies[m]:
            copy.wait()
        low, mid, high = (wbuf[m, dr * deep : (dr + 1) * deep, :] for dr in range(3))
        outer = low + high
        hbuf[m, :deep, :] = outer + mid
        hbuf[m, deep:, :] = outer - mid
        parts = []
        for n in range(4):
            k = 4 * m + n
            left = jnp.concatenate(
                [xa[k, 0:OUT_HALF, :], xa[k, HL // 2 : HL // 2 + OUT_HALF, :], xa[k, HL : HL + OUT_HALF, :]], axis=-1
            )
            right = hbuf[m, (n - 1) * deep : n * deep, :] if n in (1, 2) else wbuf[m, n // 3 * 2 * deep : (n // 3 * 2 + 1) * deep, :]
            parts.append(jnp.dot(left, right, preferred_element_type=f32))
        middle = (
            parts[0] + 0.5 * (parts[1] + parts[2]),
            0.5 * (parts[1] - parts[2]) - parts[3],
        )
        for p in range(2):
            if m == 0:
                ysum[0, p] = middle[p]
            elif m == 1:
                ysum[0, p] += middle[p]
                ysum[1, p] = same * middle[p]
            elif m == 2:
                ysum[0, p] += middle[p]
                ysum[1, p] -= same * middle[p]
            else:
                ysum[1, p] += middle[p]

    hgain = 0.5 * hg_ref[...].reshape(1, CH)
    lane = lax.broadcasted_iota(jnp.int32, (HL // 2, LANE), 1)
    for t in range(2):
        for p in range(2):
            rest = jnp.concatenate(
                [
                    jnp.concatenate(
                        [first[t, col, lt, pl.ds(p, HL // 2, stride=2), :] for lt in range(LT)], axis=-1
                    )
                    for col in range(1, 1 + OUT_COLS)
                ],
                axis=0,
            )
            x = ysum[t, p] + rest
            outward = silu_of_twice(x * inv_rms(x) * hgain).astype(bf16)
            patch = lax.dot_general(outward, hwbuf[...], (((1,), (1,)), ((), ())), preferred_element_type=f32)
            for colour in range(3):
                sums = [jnp.zeros((HL // 2, LANE), f32), jnp.zeros((HL // 2, LANE), f32)]
                for w in range(-1, WS):
                    cell = patch[(w + 1) * HL // 2 : (w + 2) * HL // 2]
                    if w < 0:
                        cell = cell * inner_left
                    turned = pltpu.roll(cell, (8 * w - PATCH * colour) % LANE, 1)
                    inside = (lane >= 8 * w) & (lane < 8 * w + PATCH)
                    sums[w % 2] = jnp.where(inside, turned, sums[w % 2])
                out_ref[0, t, colour, pl.ds(p, HL // 2, stride=2), :] = sums[0] + sums[1]


def window_kernel(tiles, latents_ref, out_ref, columns, packed_ref, moved):
    count, rows = packed_ref.shape[0], packed_ref.shape[1]
    flat = latents_ref[...].astype(jnp.float32).reshape(rows * CLAT, count * PER_TILE)
    for at in range(0, rows * CLAT, LANE):
        wide = min(LANE, rows * CLAT - at)
        columns[at // LANE, :, :wide] = flat[at : at + wide].T
    lane = lax.broadcasted_iota(jnp.int32, (count, LANE), 1)
    for row in range(rows):
        at = row * CLAT
        total = jnp.zeros((count, LANE), jnp.float32)
        for within in range(PER_TILE):
            piece = columns[at // LANE, pl.ds(within, count, stride=PER_TILE), :]
            piece = pltpu.roll(piece, (within * CLAT - at) % LANE, 1)
            total = jnp.where((lane >= within * CLAT) & (lane < (within + 1) * CLAT), piece, total)
        packed_ref[:, row, :] = total
    lane = lax.broadcasted_iota(jnp.int32, (rows, LANE), 1)
    turned = [jnp.zeros((rows, LANE), jnp.float32)]
    for tile in range(count):
        turned.append(pltpu.roll(packed_ref[tile], LANE - SKIP, 1))
    turned.append(jnp.zeros((rows, LANE), jnp.float32))
    for tile in range(count + 1):
        moved[tile] = jnp.where(lane < LANE - SKIP, turned[tile], turned[tile + 1]).astype(out_ref.dtype)
    for dest in range(tiles):
        strip = (dest - (STRIPS // 2 - 1)) % tiles % STRIPS
        for tile in range(TILES_WIN):
            if 2 * strip + tile <= count:
                out_ref[dest, tile * rows : (tile + 1) * rows] = moved[2 * strip + tile]
            else:
                out_ref[dest, tile * rows : (tile + 1) * rows] = jnp.zeros((rows, LANE), out_ref.dtype)


def per_device(latents, clip_index, first_conv, first_gain, middle_conv, head_gain, head_weight):
    tiles = lax.axis_size("tile")
    place = lax.axis_index("tile").astype(jnp.int32).reshape(1)
    rows = latents.shape[0]
    width = latents.shape[2]
    blocks = tiles // STRIPS
    slots = min(6, blocks * TF)
    sent = pl.pallas_call(
        functools.partial(window_kernel, tiles),
        out_shape=jax.ShapeDtypeStruct((tiles, TILES_WIN * rows, LANE), latents.dtype),
        in_specs=[pl.BlockSpec(memory_space=pltpu.VMEM)],
        out_specs=pl.BlockSpec(memory_space=pltpu.VMEM),
        scratch_shapes=[
            pltpu.VMEM((pl.cdiv(rows * CLAT, LANE), width, LANE), jnp.float32),
            pltpu.VMEM((width // PER_TILE, rows, LANE), jnp.float32),
            pltpu.VMEM((width // PER_TILE + 1, rows, LANE), latents.dtype),
        ],
        compiler_params=pltpu.CompilerParams(vmem_limit_bytes=8 * 1024 * 1024),
    )(latents)
    came = lax.all_to_all(sent, "tile", 0, 0, tiled=True)

    vmem = pl.BlockSpec(memory_space=pltpu.VMEM)
    smem = pl.BlockSpec(memory_space=pltpu.SMEM)
    anywhere = pl.BlockSpec(memory_space=pl.ANY)
    weights, b1 = pl.pallas_call(
        functools.partial(weights_kernel, tiles),
        out_shape=(
            jax.ShapeDtypeStruct((2, 9 * CH, CH), jnp.bfloat16),
            jax.ShapeDtypeStruct((3, 12 * CLAT, 2 * CH), jnp.bfloat16),
        ),
        in_specs=[
            smem,
            smem,
            anywhere,
            vmem,
        ],
        out_specs=(anywhere, vmem),
        scratch_shapes=[
            pltpu.VMEM((3, 3, 3, CH, CH), jnp.bfloat16),
            pltpu.VMEM((9, 2, CH, CH), jnp.bfloat16),
            pltpu.SemaphoreType.DMA((3,)),
            pltpu.SemaphoreType.DMA((18,)),
        ],
        compiler_params=pltpu.CompilerParams(vmem_limit_bytes=67_043_328),
        cost_estimate=pl.CostEstimate(flops=20_000_000, bytes_accessed=15_000_000, transcendentals=0),
    )(place, clip_index, middle_conv, first_conv)

    return pl.pallas_call(
        functools.partial(decode_kernel, slots),
        out_shape=jax.ShapeDtypeStruct((1, TF, 3, HL, WS * PATCH // 2), jnp.float32),
        in_specs=[smem, smem, vmem, vmem, vmem, anywhere, anywhere, vmem, vmem],
        out_specs=vmem,
        scratch_shapes=[
            pltpu.VMEM((4, 9 * CH, CH), jnp.bfloat16),
            pltpu.VMEM((4, 6 * CH, CH), jnp.bfloat16),
            pltpu.VMEM((LANE, CH), jnp.bfloat16),
            pltpu.VMEM((HL + 2 * PAD, TILES_WIN * LANE), jnp.float32),
            pltpu.VMEM((slots, CELLS, 192), jnp.bfloat16),
            pltpu.VMEM((4, COLS, LT, HL + 2 * PAD, LANE), jnp.float32),
            pltpu.VMEM((2, COLS, LT, HL, LANE), jnp.float32),
            pltpu.VMEM((16, CELLS, CH), jnp.bfloat16),
            pltpu.VMEM((2, 2, OUT_HALF, CH), jnp.float32),
            pltpu.SemaphoreType.DMA((36,)),
        ],
        compiler_params=pltpu.CompilerParams(vmem_limit_bytes=67_043_328),
    )(
        place,
        clip_index,
        came,
        b1,
        first_gain,
        weights,
        middle_conv,
        head_gain,
        head_weight.T,
    )


def solution(mesh):
    placed = (P(("group", "tile"), None, None), P("group"), P(), P(), P(), P(), P())
    return jax.shard_map(
        per_device,
        mesh=mesh,
        in_specs=placed,
        out_specs=P(("group", "tile"), None, None, None, None),
        check_vma=False,
    )
```

```python
import functools

import jax
import jax.numpy as jnp
from jax import lax
from jax.experimental import pallas as pl
from jax.experimental.pallas import tpu as pltpu
from jax.sharding import PartitionSpec as P

CLAT = 16
CH = 384
PATCH = 16
STRIPS = 8
TF = 2
WS = 16
HL = 48
LANE = 128
PER_TILE = LANE // CLAT
TILES_WIN = 3
SKIP = (PER_TILE - 3) * CLAT
PAIRS = 10
COLS = 2 * PAIRS
OUT_COLS = WS + 1
CELLS = PAIRS * HL
OUT_HALF = OUT_COLS * HL // 2
PAD = 8
STEP = 64
LT = CH // LANE


def silu_of_twice(half):
    return half + half * jnp.tanh(half)


def inv_rms(x):
    return lax.rsqrt(jnp.mean(x * x, axis=-1, keepdims=True) + 1e-06)


def position(place_ref, tiles):
    rotated = lax.rem(place_ref[0] - (STRIPS // 2 - 1) + tiles, tiles)
    return lax.rem(rotated, STRIPS), lax.div(rotated, STRIPS)


def frame_ids(clip_ref, block):
    ids = []
    for slot in range(6):
        frame = block * TF - 4 + slot
        known = clip_ref[jnp.maximum(frame, 0)]
        ids.append(jnp.where(frame >= 0, known, -1))
    return ids


def flag(condition):
    return jnp.where(condition, 1.0, 0.0).astype(jnp.float32)


def weights_kernel(tiles, place_ref, clip_ref, mc_ref, fc_ref, out_ref, b1_ref, gbuf, mbuf, insem, outsem):
    f32, bf16 = jnp.float32, jnp.bfloat16
    loads = []
    for dr in range(3):
        load = pltpu.make_async_copy(mc_ref.at[:, dr], gbuf.at[:, dr], insem.at[dr])
        load.start()
        loads.append(load)
    _, block = position(place_ref, tiles)
    ids = frame_ids(clip_ref, block)
    same = flag(ids[4] == ids[5])
    scale = 1.0 - 0.5 * same

    b1_ref[...] = jnp.zeros_like(b1_ref)
    for dt in range(3):
        for dr in range(3):
            for dc in range(3):
                at = dr * 64 + dc * CLAT
                taps = fc_ref[dt, dr, dc]
                b1_ref[dt, at : at + CLAT, :CH] = taps
                b1_ref[dt, at + CLAT : at + 2 * CLAT, CH:] = taps

    stores = []
    for dr in range(3):
        loads[dr].wait()
        for dc in range(3):
            tap = dr * 3 + dc

            def rows(i, carry):
                at = pl.multiple_of(i * STEP, STEP)
                g0, g1, g2 = (gbuf[dt, dr, dc, pl.ds(at, STEP), :].astype(f32) for dt in range(3))
                s0 = same * g0
                mbuf[tap, 0, pl.ds(at, STEP), :] = (scale * (g1 + (s0 + same * g2))).astype(bf16)
                mbuf[tap, 1, pl.ds(at, STEP), :] = (scale * (g2 + (s0 - same * g1))).astype(bf16)
                return carry

            lax.fori_loop(0, CH // STEP, rows, 0)
            for m in range(2):
                store = pltpu.make_async_copy(
                    mbuf.at[tap, m], out_ref.at[m, pl.ds(tap * CH, CH)], outsem.at[tap * 2 + m]
                )
                store.start()
                stores.append(store)
    for store in stores:
        store.wait()


def decode_kernel(
    slots,
    place_ref,
    clip_ref,
    recv_ref,
    b1_ref,
    fg_ref,
    wt_ref,
    mc_ref,
    hg_ref,
    hw_ref,
    out_ref,
    wbuf,
    hbuf,
    hwbuf,
    vf,
    x1,
    act,
    first,
    xa,
    ysum,
    wsem,
):
    f32, bf16 = jnp.float32, jnp.bfloat16
    copies = []
    for m in range(4):
        group = []
        for dr in range(3):
            for dc in range(3):
                tap = pl.ds((dr * 3 + dc) * CH, CH)
                source = mc_ref.at[m // 3 * 2, dr, dc] if m in (0, 3) else wt_ref.at[m - 1, tap]
                copy = pltpu.make_async_copy(source, wbuf.at[m, tap], wsem.at[m * 9 + dr * 3 + dc])
                copy.start()
                group.append(copy)
        copies.append(group)

    column, block = position(place_ref, recv_ref.shape[0])
    ids = frame_ids(clip_ref, block)
    inner_left = flag(column > 0)
    inner_right = flag(column < STRIPS - 1)
    hwbuf[...] = jnp.zeros_like(hwbuf)
    hwbuf[: 3 * PATCH] = hw_ref[...]

    vf[...] = jnp.zeros_like(vf)
    for slot in range(6 - slots, 6):
        base = jnp.maximum(block * TF - 4 + slot, 0) * 4
        for quarter in range(4):
            for tile in range(TILES_WIN):
                vf[PAD + 12 * quarter : PAD + 12 * quarter + 12, tile * LANE : (tile + 1) * LANE] = (
                    recv_ref[base + quarter, 12 * tile : 12 * tile + 12].astype(f32)
                )
        rows = [vf[PAD - 1 + dr : PAD - 1 + dr + HL, :] for dr in range(3)]
        for pair in range(PAIRS):
            at = 32 * pair
            x1[slot - 6 + slots, pair * HL : (pair + 1) * HL, :] = jnp.concatenate(
                [row[:, at : at + 64] for row in rows], axis=-1
            ).astype(bf16)

    for t in range(4):
        for col in range(COLS):
            for lt in range(LT):
                act[t, col, lt, 0:PAD, :] = jnp.zeros((PAD, LANE), f32)
                act[t, col, lt, PAD + HL :, :] = jnp.zeros((PAD, LANE), f32)
    gain = 0.5 * fg_ref[...].reshape(1, CH)
    same = flag(ids[4] == ids[5])
    keeps = [flag(ids[2] == ids[4]), flag(ids[3] == ids[4]), None, None]
    for t in range(4):
        total = None
        for dt in range(3):
            slot = t + dt
            if slot < 6 - slots:
                continue
            left = x1[slot - 6 + slots]
            if dt < 2:
                left = left * flag(ids[slot] == ids[t + 2]).astype(bf16)
            part = jnp.dot(left, b1_ref[dt], preferred_element_type=f32)
            total = part if total is None else total + part
        for side in range(2):
            x = total[:, side * CH : (side + 1) * CH]
            a = silu_of_twice(x * inv_rms(x) * (gain if keeps[t] is None else gain * keeps[t]))
            for pair in range(PAIRS):
                cut = slice(pair * HL, (pair + 1) * HL)
                piece = a[cut]
                if pair == 0:
                    piece = piece * inner_left
                if pair == PAIRS - 1:
                    piece = piece * inner_right
                for lt in range(LT):
                    lanes = slice(lt * LANE, (lt + 1) * LANE)
                    act[t, 2 * pair + side, lt, PAD : PAD + HL, :] = piece[:, lanes]
                    if t >= 2:
                        first[t - 2, 2 * pair + side, lt] = x[cut, lanes]

    def transform(pair, carry):
        at = pl.multiple_of(pair * HL, HL)
        for lt in range(LT):
            sides = []
            for side in range(2):
                timed = []
                for k in range(4):
                    d = [act[t, 2 * pair + side, lt, pl.ds(PAD - 1 + k, HL // 2, stride=2), :] for t in range(4)]
                    s1, s2 = same * d[1], same * d[2]
                    timed.append((d[0] - s2, d[1] + s2, d[2] - s1, d[3] - s1))
                mixed = []
                for m in range(4):
                    r0, r1, r2, r3 = (timed[k][m] for k in range(4))
                    mixed += [r0 - r2, r1 + r2, r2 - r1, r1 - r3]
                sides.append(mixed)
            for k in range(16):
                both = jnp.concatenate([sides[0][k], sides[1][k]], axis=0).astype(bf16)
                xa[k, pl.ds(at, HL), lt * LANE : (lt + 1) * LANE] = both
        return carry

    lax.fori_loop(0, PAIRS, transform, 0, unroll=5)

    deep = 3 * CH
    for m in range(4):
        for copy in copies[m]:
            copy.wait()
        low, mid, high = (wbuf[m, dr * deep : (dr + 1) * deep, :] for dr in range(3))
        outer = low + high
        hbuf[m, :deep, :] = outer + mid
        hbuf[m, deep:, :] = outer - mid
        parts = []
        for n in range(4):
            k = 4 * m + n
            left = jnp.concatenate(
                [xa[k, 0:OUT_HALF, :], xa[k, HL // 2 : HL // 2 + OUT_HALF, :], xa[k, HL : HL + OUT_HALF, :]], axis=-1
            )
            right = hbuf[m, (n - 1) * deep : n * deep, :] if n in (1, 2) else wbuf[m, n // 3 * 2 * deep : (n // 3 * 2 + 1) * deep, :]
            parts.append(jnp.dot(left, right, preferred_element_type=f32))
        middle = (
            parts[0] + 0.5 * (parts[1] + parts[2]),
            0.5 * (parts[1] - parts[2]) - parts[3],
        )
        for p in range(2):
            if m == 0:
                ysum[0, p] = middle[p]
            elif m == 1:
                ysum[0, p] += middle[p]
                ysum[1, p] = same * middle[p]
            elif m == 2:
                ysum[0, p] += middle[p]
                ysum[1, p] -= same * middle[p]
            else:
                ysum[1, p] += middle[p]

    hgain = 0.5 * hg_ref[...].reshape(1, CH)
    lane = lax.broadcasted_iota(jnp.int32, (HL // 2, LANE), 1)
    for t in range(2):
        for p in range(2):
            rest = jnp.concatenate(
                [
                    jnp.concatenate(
                        [first[t, col, lt, pl.ds(p, HL // 2, stride=2), :] for lt in range(LT)], axis=-1
                    )
                    for col in range(1, 1 + OUT_COLS)
                ],
                axis=0,
            )
            x = ysum[t, p] + rest
            outward = silu_of_twice(x * inv_rms(x) * hgain).astype(bf16)
            patch = lax.dot_general(outward, hwbuf[...], (((1,), (1,)), ((), ())), preferred_element_type=f32)
            for colour in range(3):
                sums = [jnp.zeros((HL // 2, LANE), f32), jnp.zeros((HL // 2, LANE), f32)]
                for w in range(-1, WS):
                    cell = patch[(w + 1) * HL // 2 : (w + 2) * HL // 2]
                    if w < 0:
                        cell = cell * inner_left
                    turned = pltpu.roll(cell, (8 * w - PATCH * colour) % LANE, 1)
                    inside = (lane >= 8 * w) & (lane < 8 * w + PATCH)
                    sums[w % 2] = jnp.where(inside, turned, sums[w % 2])
                out_ref[0, t, colour, pl.ds(p, HL // 2, stride=2), :] = sums[0] + sums[1]


def window_kernel(tiles, latents_ref, out_ref, columns, packed_ref, moved):
    count, rows = packed_ref.shape[0], packed_ref.shape[1]
    flat = latents_ref[...].astype(jnp.float32).reshape(rows * CLAT, count * PER_TILE)
    for at in range(0, rows * CLAT, LANE):
        wide = min(LANE, rows * CLAT - at)
        columns[at // LANE, :, :wide] = flat[at : at + wide].T
    lane = lax.broadcasted_iota(jnp.int32, (count, LANE), 1)
    for row in range(rows):
        at = row * CLAT
        total = jnp.zeros((count, LANE), jnp.float32)
        for within in range(PER_TILE):
            piece = columns[at // LANE, pl.ds(within, count, stride=PER_TILE), :]
            piece = pltpu.roll(piece, (within * CLAT - at) % LANE, 1)
            total = jnp.where((lane >= within * CLAT) & (lane < (within + 1) * CLAT), piece, total)
        packed_ref[:, row, :] = total
    lane = lax.broadcasted_iota(jnp.int32, (rows, LANE), 1)
    turned = [jnp.zeros((rows, LANE), jnp.float32)]
    for tile in range(count):
        turned.append(pltpu.roll(packed_ref[tile], LANE - SKIP, 1))
    turned.append(jnp.zeros((rows, LANE), jnp.float32))
    for tile in range(count + 1):
        moved[tile] = jnp.where(lane < LANE - SKIP, turned[tile], turned[tile + 1]).astype(out_ref.dtype)
    for dest in range(tiles):
        strip = (dest - (STRIPS // 2 - 1)) % tiles % STRIPS
        for tile in range(TILES_WIN):
            if 2 * strip + tile <= count:
                out_ref[dest, tile * rows : (tile + 1) * rows] = moved[2 * strip + tile]
            else:
                out_ref[dest, tile * rows : (tile + 1) * rows] = jnp.zeros((rows, LANE), out_ref.dtype)


def per_device(latents, clip_index, first_conv, first_gain, middle_conv, head_gain, head_weight):
    tiles = lax.axis_size("tile")
    place = lax.axis_index("tile").astype(jnp.int32).reshape(1)
    rows = latents.shape[0]
    width = latents.shape[2]
    blocks = tiles // STRIPS
    slots = min(6, blocks * TF)
    sent = pl.pallas_call(
        functools.partial(window_kernel, tiles),
        out_shape=jax.ShapeDtypeStruct((tiles, TILES_WIN * rows, LANE), latents.dtype),
        in_specs=[pl.BlockSpec(memory_space=pltpu.VMEM)],
        out_specs=pl.BlockSpec(memory_space=pltpu.VMEM),
        scratch_shapes=[
            pltpu.VMEM((pl.cdiv(rows * CLAT, LANE), width, LANE), jnp.float32),
            pltpu.VMEM((width // PER_TILE, rows, LANE), jnp.float32),
            pltpu.VMEM((width // PER_TILE + 1, rows, LANE), latents.dtype),
        ],
        compiler_params=pltpu.CompilerParams(vmem_limit_bytes=8 * 1024 * 1024),
    )(latents)
    came = lax.all_to_all(sent, "tile", 0, 0, tiled=True)

    vmem = pl.BlockSpec(memory_space=pltpu.VMEM)
    smem = pl.BlockSpec(memory_space=pltpu.SMEM)
    anywhere = pl.BlockSpec(memory_space=pl.ANY)
    weights, b1 = pl.pallas_call(
        functools.partial(weights_kernel, tiles),
        out_shape=(
            jax.ShapeDtypeStruct((2, 9 * CH, CH), jnp.bfloat16),
            jax.ShapeDtypeStruct((3, 12 * CLAT, 2 * CH), jnp.bfloat16),
        ),
        in_specs=[
            smem,
            smem,
            anywhere,
            vmem,
        ],
        out_specs=(anywhere, vmem),
        scratch_shapes=[
            pltpu.VMEM((3, 3, 3, CH, CH), jnp.bfloat16),
            pltpu.VMEM((9, 2, CH, CH), jnp.bfloat16),
            pltpu.SemaphoreType.DMA((3,)),
            pltpu.SemaphoreType.DMA((18,)),
        ],
        compiler_params=pltpu.CompilerParams(vmem_limit_bytes=67_043_328),
        cost_estimate=pl.CostEstimate(flops=20_000_000, bytes_accessed=15_000_000, transcendentals=0),
    )(place, clip_index, middle_conv, first_conv)

    return pl.pallas_call(
        functools.partial(decode_kernel, slots),
        out_shape=jax.ShapeDtypeStruct((1, TF, 3, HL, WS * PATCH // 2), jnp.float32),
        in_specs=[smem, smem, vmem, vmem, vmem, anywhere, anywhere, vmem, vmem],
        out_specs=vmem,
        scratch_shapes=[
            pltpu.VMEM((4, 9 * CH, CH), jnp.bfloat16),
            pltpu.VMEM((4, 6 * CH, CH), jnp.bfloat16),
            pltpu.VMEM((LANE, CH), jnp.bfloat16),
            pltpu.VMEM((HL + 2 * PAD, TILES_WIN * LANE), jnp.float32),
            pltpu.VMEM((slots, CELLS, 192), jnp.bfloat16),
            pltpu.VMEM((4, COLS, LT, HL + 2 * PAD, LANE), jnp.float32),
            pltpu.VMEM((2, COLS, LT, HL, LANE), jnp.float32),
            pltpu.VMEM((16, CELLS, CH), jnp.bfloat16),
            pltpu.VMEM((2, 2, OUT_HALF, CH), jnp.float32),
            pltpu.SemaphoreType.DMA((36,)),
        ],
        compiler_params=pltpu.CompilerParams(vmem_limit_bytes=67_043_328),
    )(
        place,
        clip_index,
        came,
        b1,
        first_gain,
        weights,
        middle_conv,
        head_gain,
        head_weight.T,
    )


def solution(mesh):
    placed = (P(("group", "tile"), None, None), P("group"), P(), P(), P(), P(), P())
    return jax.shard_map(
        per_device,
        mesh=mesh,
        in_specs=placed,
        out_specs=P(("group", "tile"), None, None, None, None),
        check_vma=False,
    )
```
